32 devices in a mesh: dp: 8 (over y, x, core), seq: 4 (over z).
Axes of the slice: x: 2, y: 2, z: 4, core: 2. Of those that a mesh axis runs over, the one named last changes fastest.
Arguments:
- queries: bfloat16 [8192, 1664], P(('dp', 'seq')), parts along dimension 0, may hold values from -6 to 6
- key_rows: bfloat16 [8192, 1664], P(('dp', 'seq')), parts along dimension 0, may hold values from -6 to 6
- value_rows: bfloat16 [8192, 1664], P(('dp', 'seq')), parts along dimension 0, may hold values from -6 to 6
Outputs:
- merged_tokens: bfloat16 [2048, 6656], P('dp', 'seq'), parts along dimension 0
The draws below stay inside these ranges and needn't reach their ends.
There are 8 independent parts, one for each index of `dp`. The reference program is written for one: setup_inputs(seed, part) draws one part's arguments, and reference() takes and returns one part's arrays. A program takes and returns all parts, laid end to end along the dimension named above; each array names one. Nothing has to cross between parts.
All inputs are finite; a program needn't handle non-finite values.
Results may differ from the reference program's by a relative error of at most 0.005.
Values may be sent and summed in bfloat16 or wider, within the bound.
A program may use at most 128 MiB of HBM per device.

```python
import math
import jax
import jax.numpy as jnp
from jax import lax

HEADS = 13
HEAD_DIM = 128
GRID_W = 64
TOKENS = 1024
CH = 1664


def draw_pair(key):
    width = HEADS * HEAD_DIM
    query_key = jax.random.fold_in(key, 11)
    other_key = jax.random.fold_in(key, 12)
    queries = 1.6 * jax.random.truncated_normal(query_key, -3.75, 3.75, (TOKENS, width), jnp.float32)
    key_rows = 1.6 * jax.random.truncated_normal(other_key, -3.75, 3.75, (TOKENS, width), jnp.float32)
    return (queries, key_rows)


def draw_queries(key, part):
    return draw_pair(key)[0].astype(jnp.bfloat16)


def draw_key_rows(key, part):
    return draw_pair(key)[1].astype(jnp.bfloat16)


def block_levels(stream_key, shape, split, least, top_value):
    loudness, own = 1.0, jax.random.fold_in(stream_key, 6)
    for axis_at, blocks in split:
        heights = jnp.exp(jax.random.uniform(jax.random.fold_in(own, axis_at), (blocks,), jnp.float32, least / len(split), top_value / len(split)))
        loudness = loudness * jnp.repeat(heights, shape[axis_at] // blocks).reshape([-1 if axis == axis_at else 1 for axis in range(len(shape))])
    return loudness


def centred(own_key, extent, spread, limit, pieces=(), dtype=jnp.bfloat16):
    gain = block_levels(own_key, extent, pieces, -0.22, 0.18) if pieces else 1.0
    drawn = jax.random.normal(own_key, extent, jnp.float32) * spread * gain
    return jnp.minimum(jnp.maximum(drawn, -limit), limit).astype(dtype)


def setup_inputs(seed: int = 0, part: int = 0) -> dict:
    keys = jax.random.split(jax.random.key(seed), 4)
    own_keys = jax.random.split(jax.random.fold_in(keys[3], part), 4)
    queries = draw_queries(jax.random.fold_in(jax.random.fold_in(keys[3], part), 71), part)
    key_rows = draw_key_rows(jax.random.fold_in(jax.random.fold_in(keys[3], part), 71), part)
    value_rows = centred(own_keys[2], (TOKENS, CH), 1.0, 6.0, ((0, 4),))
    return {"queries": queries, "key_rows": key_rows, "value_rows": value_rows}


def one_head(query_head, key_head, value_head):
    total_rows = query_head.shape[0]
    block_rows = math.gcd(total_rows, 512)
    score_scale = 1.0 / math.sqrt(HEAD_DIM)
    blocks = query_head.reshape(total_rows // block_rows, block_rows, HEAD_DIM)

    def attend(query_block):
        scores = jnp.dot(query_block, key_head.T, preferred_element_type=jnp.float32) * score_scale
        row_max = lax.optimization_barrier(jnp.max(scores, axis=-1, keepdims=True))
        weights = jnp.exp(scores - row_max)
        totals = lax.optimization_barrier(jnp.sum(weights, axis=-1, keepdims=True))
        weighted = jnp.dot(weights.astype(jnp.bfloat16), value_head, preferred_element_type=jnp.float32)
        return (weighted / totals).astype(jnp.bfloat16)
    return lax.map(attend, blocks).reshape(total_rows, HEAD_DIM)

def reference(queries, key_rows, value_rows):
    tokens = queries.shape[0]
    query_heads = queries.reshape(tokens, HEADS, HEAD_DIM).transpose(1, 0, 2)
    key_heads = key_rows.reshape(tokens, HEADS, HEAD_DIM).transpose(1, 0, 2)
    value_heads = value_rows.reshape(tokens, HEADS, HEAD_DIM).transpose(1, 0, 2)
    attended = lax.map(lambda triple: one_head(triple[0], triple[1], triple[2]), (query_heads, key_heads, value_heads))
    attended = attended.transpose(1, 0, 2).reshape(tokens, HEADS * HEAD_DIM)
    grid_rows = tokens // GRID_W
    shuffled = attended.reshape(grid_rows // 2, 2, GRID_W // 2, 2, HEADS * HEAD_DIM).transpose(0, 2, 1, 3, 4)
    return shuffled.reshape(grid_rows // 2 * (GRID_W // 2), 4 * HEADS * HEAD_DIM)
```

```python
import functools
import math

import jax
import jax.numpy as jnp
from jax import lax
from jax.experimental import pallas as pl
from jax.experimental.pallas import tpu as pltpu
from jax.sharding import PartitionSpec as P

HEAD_DIM = 128
GRID_W = 64
MERGE = 2


def by_heads(queries, key_rows, value_rows, score_scale):
    tok_rows, width = queries.shape
    heads = width // HEAD_DIM
    groups = lax.axis_size("seq")
    padded_heads = -(-heads // groups) * groups

    def spread(source):
        shaped = source.reshape(tok_rows, heads, HEAD_DIM)
        shaped = jnp.pad(shaped, ((0, 0), (0, padded_heads - heads), (0, 0)))
        return shaped.reshape(tok_rows, groups, padded_heads // groups, HEAD_DIM)

    head_query = lax.all_to_all(spread(queries), "seq", split_axis=1, concat_axis=0, tiled=True)
    head_key = lax.all_to_all(spread(key_rows), "seq", split_axis=1, concat_axis=0, tiled=True)
    head_value = lax.all_to_all(spread(value_rows), "seq", split_axis=1, concat_axis=0, tiled=True)
    total_rows = head_query.shape[0]
    head_count = head_query.shape[2]
    flat_key = head_key.reshape(total_rows, head_count, HEAD_DIM)
    flat_value = head_value.reshape(total_rows, head_count, HEAD_DIM)
    step_rows = math.gcd(total_rows, 512)
    blocks = head_query.reshape(total_rows // step_rows, step_rows, head_count, HEAD_DIM)

    def one_block(query_block):
        scores = (
            jnp.einsum("qhd,khd->hqk", query_block, flat_key, preferred_element_type=jnp.float32)
            * score_scale
        )
        row_max = jnp.max(scores, axis=-1, keepdims=True)
        weights = jnp.exp(scores - row_max)
        totals = jnp.sum(weights, axis=-1, keepdims=True)
        weighted = jnp.einsum(
            "hqk,khd->qhd",
            weights.astype(jnp.bfloat16),
            flat_value,
            preferred_element_type=jnp.float32,
        )
        return (weighted / totals.transpose(1, 0, 2)).astype(jnp.bfloat16)

    result = lax.map(one_block, blocks).reshape(total_rows, 1, head_count, HEAD_DIM)
    result = lax.all_to_all(result, "seq", split_axis=0, concat_axis=1, tiled=True)
    return result.reshape(tok_rows, padded_heads, HEAD_DIM)[:, :heads].reshape(tok_rows, width)


def split_features(queries, key_rows, value_rows):
    score_scale = 1.0 / math.sqrt(HEAD_DIM)
    attended = by_heads(queries, key_rows, value_rows, score_scale)
    tok_rows, width = attended.shape
    grid_rows = tok_rows // GRID_W
    shuffled = attended.reshape(grid_rows // 2, 2, GRID_W // 2, 2, width).transpose(0, 2, 1, 3, 4)
    shuffled = shuffled.reshape(grid_rows // 2 * (GRID_W // 2), 4 * width)
    return lax.all_to_all(shuffled, "seq", split_axis=1, concat_axis=0, tiled=True)


def head_kernel(
    n, heads, query_rows,
    q_ref, k_ref, v_ref, out_ref,
    held, obuf, osend,
    landed, sent, merged, ready, far, everyone,
):
    me = lax.axis_index("seq")
    flip = lax.rem(lax.axis_index("dp"), 2)
    base, extra = heads // n, heads % n
    lead = 1 if extra else 0
    slots = base + lead
    rows = q_ref.shape[0]
    total_rows = rows * n
    score_scale = 1.0 / math.sqrt(HEAD_DIM)

    def place(device):
        return flip * (n - 1 - device) + (1 - flip) * device

    def head_of(device, slot):
        at = place(device)
        regular = at * base + slot - lead
        if not lead:
            return regular
        return jnp.where(slot == 0, n * base + at, regular)

    def has(device, slot):
        if not lead:
            return slot >= 0
        return jnp.logical_or(slot > 0, place(device) < extra)

    def columns(head):
        return pl.ds(pl.multiple_of(head * HEAD_DIM, HEAD_DIM), HEAD_DIM)

    def rows_of(tensor, device):
        return pl.ds(pl.multiple_of(tensor * total_rows + device * rows, rows), rows)

    peers = (n - 1 - me, lax.rem(me + n // 2, n), me + 1 - 2 * lax.rem(me, 2))
    tensors = (k_ref, q_ref, v_ref)

    def inward(t, slot, peer):
        return pltpu.make_async_remote_copy(
            src_ref=tensors[t].at[:, columns(head_of(peer, slot))],
            dst_ref=held.at[slot, rows_of(t, me), :],
            send_sem=sent,
            recv_sem=landed.at[slot],
            device_id={"seq": peer},
            device_id_type=pl.DeviceIdType.MESH,
        )

    def inward_own(t, slot):
        return pltpu.make_async_copy(
            tensors[t].at[:, columns(head_of(me, slot))],
            held.at[slot, rows_of(t, me), :],
            landed.at[slot],
        )

    def outward(slot, peer):
        return pltpu.make_async_remote_copy(
            src_ref=osend.at[slot, peer],
            dst_ref=out_ref.at[:, columns(head_of(me, slot))],
            send_sem=sent,
            recv_sem=merged,
            device_id={"seq": peer},
            device_id_type=pl.DeviceIdType.MESH,
        )

    def outward_own(slot):
        return pltpu.make_async_copy(
            osend.at[slot, me], out_ref.at[:, columns(head_of(me, slot))], merged
        )

    def wait_bytes(ref, sem):
        pltpu.make_async_copy(ref, ref, sem).wait()

    partner, mate = peers[0], peers[2]
    inner = (me > 0) & (me < n - 1)
    early = lead + 1

    def tell(sem, device):
        pl.semaphore_signal(
            sem, inc=1, device_id={"seq": device}, device_id_type=pl.DeviceIdType.MESH
        )

    barrier = pltpu.get_barrier_semaphore()

    @pl.when(inner)
    def _():
        tell(barrier, partner)
        tell(barrier, mate)

    pl.semaphore_wait(barrier, 1)

    @pl.when(inner)
    def _():
        for slot in range(early):
            for t in range(3):
                @pl.when(has(partner, slot))
                def _():
                    inward(t, slot, partner).start()
        pl.semaphore_wait(ready, 1)
        tell(far, partner)
        pl.semaphore_wait(far, 1)
        tell(everyone, mate)

    @pl.when(jnp.logical_not(inner))
    def _():
        tell(ready, mate)
        pl.semaphore_wait(everyone, 1)

    @pl.loop(0, slots)
    def _(slot):
        for t in range(3):
            for peer in peers:
                fresh = has(peer, slot)
                if peer is partner:
                    fresh = fresh & ((slot >= early) | jnp.logical_not(inner))

                @pl.when(fresh)
                def _():
                    inward(t, slot, peer).start()

            @pl.when(has(me, slot))
            def _():
                inward_own(t, slot).start()

    @pl.loop(0, slots)
    def _(slot):
        @pl.when(has(me, slot))
        def _():
            wait_bytes(held.at[slot], landed.at[slot])

            @pl.loop(0, total_rows // query_rows)
            def _(block):
                at = pl.ds(pl.multiple_of(block * query_rows, query_rows), query_rows)
                from_q = pl.ds(pl.multiple_of(total_rows + block * query_rows, query_rows), query_rows)
                scores = lax.dot_general(
                    held[slot, from_q, :], held[slot, pl.ds(0, total_rows), :], (((1,), (1,)), ((), ())),
                    preferred_element_type=jnp.float32,
                ) * score_scale
                row_max = jnp.max(scores, axis=-1, keepdims=True)
                weights = jnp.exp(scores - row_max)
                totals = jnp.sum(weights, axis=-1, keepdims=True)
                weighted = jnp.dot(
                    weights.astype(jnp.bfloat16), held[slot, pl.ds(2 * total_rows, total_rows), :],
                    preferred_element_type=jnp.float32,
                )
                obuf[at, :] = weighted / totals

            half = GRID_W // MERGE
            for a in range(MERGE):
                for b in range(MERGE):
                    for i in range(total_rows // GRID_W // MERGE):
                        part = obuf[pl.ds((MERGE * i + a) * GRID_W + b, half, stride=MERGE), :]
                        osend[slot, MERGE * a + b, i * half:(i + 1) * half, :] = part.astype(jnp.bfloat16)
            for peer in reversed(peers):
                outward(slot, peer).start()
            outward_own(slot).start()

    wait_bytes(out_ref, merged)
    for _ in range(3):
        wait_bytes(q_ref, sent)


def on_device(queries, key_rows, value_rows):
    n = lax.axis_size("seq")
    if n != MERGE * MERGE:
        return split_features(queries, key_rows, value_rows)
    rows, width = queries.shape
    heads = width // HEAD_DIM
    slots = -(-heads // n)
    total_rows = rows * n
    merged_rows = total_rows // (MERGE * MERGE)
    anywhere = pl.BlockSpec(memory_space=pl.ANY)
    return pl.pallas_call(
        functools.partial(head_kernel, n, heads, math.gcd(total_rows, 256)),
        out_shape=pltpu.VMEM((merged_rows, width), jnp.bfloat16),
        in_specs=[anywhere] * 3,
        out_specs=pl.BlockSpec(memory_space=pltpu.VMEM),
        scratch_shapes=[
            pltpu.VMEM((slots, 3 * total_rows, HEAD_DIM), jnp.bfloat16),
            pltpu.VMEM((total_rows + 8, HEAD_DIM), jnp.float32),
            pltpu.VMEM((slots, n, merged_rows, HEAD_DIM), jnp.bfloat16),
            pltpu.SemaphoreType.DMA((slots,)),
            pltpu.SemaphoreType.DMA,
            pltpu.SemaphoreType.DMA,
            pltpu.SemaphoreType.REGULAR,
            pltpu.SemaphoreType.REGULAR,
            pltpu.SemaphoreType.REGULAR,
        ],
        compiler_params=pltpu.CompilerParams(collective_id=0, has_side_effects=True),
        name="heads_exchange",
    )(queries, key_rows, value_rows)


def solution(mesh):
    placed = (P(("dp", "seq"), None), P(("dp", "seq"), None), P(("dp", "seq"), None))
    return jax.shard_map(
        on_device, mesh=mesh, in_specs=placed, out_specs=P("dp", "seq"), check_vma=False
    )
```

```python
import functools
import math

import jax
import jax.numpy as jnp
from jax import lax
from jax.experimental import pallas as pl
from jax.experimental.pallas import tpu as pltpu
from jax.sharding import PartitionSpec as P

HEAD_DIM = 128
GRID_W = 64
MERGE = 2


def by_heads(queries, key_rows, value_rows, score_scale):
    tok_rows, width = queries.shape
    heads = width // HEAD_DIM
    groups = lax.axis_size("seq")
    padded_heads = -(-heads // groups) * groups

    def spread(source):
        shaped = source.reshape(tok_rows, heads, HEAD_DIM)
        shaped = jnp.pad(shaped, ((0, 0), (0, padded_heads - heads), (0, 0)))
        return shaped.reshape(tok_rows, groups, padded_heads // groups, HEAD_DIM)

    head_query = lax.all_to_all(spread(queries), "seq", split_axis=1, concat_axis=0, tiled=True)
    head_key = lax.all_to_all(spread(key_rows), "seq", split_axis=1, concat_axis=0, tiled=True)
    head_value = lax.all_to_all(spread(value_rows), "seq", split_axis=1, concat_axis=0, tiled=True)
    total_rows = head_query.shape[0]
    head_count = head_query.shape[2]
    flat_key = head_key.reshape(total_rows, head_count, HEAD_DIM)
    flat_value = head_value.reshape(total_rows, head_count, HEAD_DIM)
    step_rows = math.gcd(total_rows, 512)
    blocks = head_query.reshape(total_rows // step_rows, step_rows, head_count, HEAD_DIM)

    def one_block(query_block):
        scores = (
            jnp.einsum("qhd,khd->hqk", query_block, flat_key, preferred_element_type=jnp.float32)
            * score_scale
        )
        row_max = jnp.max(scores, axis=-1, keepdims=True)
        weights = jnp.exp(scores - row_max)
        totals = jnp.sum(weights, axis=-1, keepdims=True)
        weighted = jnp.einsum(
            "hqk,khd->qhd",
            weights.astype(jnp.bfloat16),
            flat_value,
            preferred_element_type=jnp.float32,
        )
        return (weighted / totals.transpose(1, 0, 2)).astype(jnp.bfloat16)

    result = lax.map(one_block, blocks).reshape(total_rows, 1, head_count, HEAD_DIM)
    result = lax.all_to_all(result, "seq", split_axis=0, concat_axis=1, tiled=True)
    return result.reshape(tok_rows, padded_heads, HEAD_DIM)[:, :heads].reshape(tok_rows, width)


def split_features(queries, key_rows, value_rows):
    score_scale = 1.0 / math.sqrt(HEAD_DIM)
    attended = by_heads(queries, key_rows, value_rows, score_scale)
    tok_rows, width = attended.shape
    grid_rows = tok_rows // GRID_W
    shuffled = attended.reshape(grid_rows // 2, 2, GRID_W // 2, 2, width).transpose(0, 2, 1, 3, 4)
    shuffled = shuffled.reshape(grid_rows // 2 * (GRID_W // 2), 4 * width)
    return lax.all_to_all(shuffled, "seq", split_axis=1, concat_axis=0, tiled=True)


def head_kernel(
    n, heads, query_rows,
    q_ref, k_ref, v_ref, out_ref,
    held, obuf, osend,
    landed, sent, merged, ready, far, everyone,
):
    me = lax.axis_index("seq")
    flip = lax.rem(lax.axis_index("dp"), 2)
    base, extra = heads // n, heads % n
    lead = 1 if extra else 0
    slots = base + lead
    rows = q_ref.shape[0]
    total_rows = rows * n
    score_scale = 1.0 / math.sqrt(HEAD_DIM)

    def place(device):
        at = device + 1 - 2 * lax.rem(device, 2)
        return flip * (n - 1 - at) + (1 - flip) * at

    def head_of(device, slot):
        at = place(device)
        regular = at * base + slot - lead
        if not lead:
            return regular
        return jnp.where(slot == 0, n * base + at, regular)

    def has(device, slot):
        if not lead:
            return slot >= 0
        return jnp.logical_or(slot > 0, place(device) < extra)

    def columns(head):
        return pl.ds(pl.multiple_of(head * HEAD_DIM, HEAD_DIM), HEAD_DIM)

    def rows_of(tensor, device):
        return pl.ds(pl.multiple_of(tensor * total_rows + device * rows, rows), rows)

    peers = (n - 1 - me, lax.rem(me + n // 2, n), me + 1 - 2 * lax.rem(me, 2))
    tensors = (k_ref, q_ref, v_ref)

    def inward(t, slot, peer):
        return pltpu.make_async_remote_copy(
            src_ref=tensors[t].at[:, columns(head_of(peer, slot))],
            dst_ref=held.at[slot, rows_of(t, me), :],
            send_sem=sent,
            recv_sem=landed.at[slot],
            device_id={"seq": peer},
            device_id_type=pl.DeviceIdType.MESH,
        )

    def inward_own(t, slot):
        return pltpu.make_async_copy(
            tensors[t].at[:, columns(head_of(me, slot))],
            held.at[slot, rows_of(t, me), :],
            landed.at[slot],
        )

    def outward(slot, peer):
        return pltpu.make_async_remote_copy(
            src_ref=osend.at[slot, peer],
            dst_ref=out_ref.at[:, columns(head_of(me, slot))],
            send_sem=sent,
            recv_sem=merged,
            device_id={"seq": peer},
            device_id_type=pl.DeviceIdType.MESH,
        )

    def outward_own(slot):
        return pltpu.make_async_copy(
            osend.at[slot, me], out_ref.at[:, columns(head_of(me, slot))], merged
        )

    def wait_bytes(ref, sem):
        pltpu.make_async_copy(ref, ref, sem).wait()

    partner, across, mate = peers
    far_low = jnp.where(me < n // 2, n // 2, 0)
    far_high = far_low + 1
    inner = (me > 0) & (me < n - 1)
    early = lead + 1

    def tell(sem, device):
        pl.semaphore_signal(
            sem, inc=1, device_id={"seq": device}, device_id_type=pl.DeviceIdType.MESH
        )

    barrier = pltpu.get_barrier_semaphore()

    @pl.when(inner)
    def _():
        tell(barrier, partner)
        tell(barrier, mate)

    pl.semaphore_wait(barrier, 1)

    @pl.when(inner)
    def _():
        for slot in range(early):
            for t in range(3):
                @pl.when(has(partner, slot))
                def _():
                    inward(t, slot, partner).start()
        pl.semaphore_wait(ready, 1)
        tell(far, partner)
        pl.semaphore_wait(far, 1)
        tell(everyone, mate)

    @pl.when(jnp.logical_not(inner))
    def _():
        tell(ready, mate)
        pl.semaphore_wait(everyone, 1)

    @pl.loop(0, slots)
    def _(slot):
        for t in range(3):
            for peer in peers:
                fresh = has(peer, slot)
                if peer is partner:
                    fresh = fresh & ((slot >= early) | jnp.logical_not(inner))

                @pl.when(fresh)
                def _():
                    inward(t, slot, peer).start()

            @pl.when(has(me, slot))
            def _():
                inward_own(t, slot).start()

    @pl.loop(0, slots)
    def _(slot):
        @pl.when(has(me, slot))
        def _():
            wait_bytes(held.at[slot], landed.at[slot])

            @pl.loop(0, total_rows // query_rows)
            def _(block):
                at = pl.ds(pl.multiple_of(block * query_rows, query_rows), query_rows)
                from_q = pl.ds(pl.multiple_of(total_rows + block * query_rows, query_rows), query_rows)
                scores = lax.dot_general(
                    held[slot, from_q, :], held[slot, pl.ds(0, total_rows), :], (((1,), (1,)), ((), ())),
                    preferred_element_type=jnp.float32,
                ) * score_scale
                row_max = jnp.max(scores, axis=-1, keepdims=True)
                weights = jnp.exp(scores - row_max)
                totals = jnp.sum(weights, axis=-1, keepdims=True)
                weighted = jnp.dot(
                    weights.astype(jnp.bfloat16), held[slot, pl.ds(2 * total_rows, total_rows), :],
                    preferred_element_type=jnp.float32,
                )
                obuf[at, :] = weighted / totals

            half = GRID_W // MERGE
            for a in range(MERGE):
                for b in range(MERGE):
                    for i in range(total_rows // GRID_W // MERGE):
                        part = obuf[pl.ds((MERGE * i + a) * GRID_W + b, half, stride=MERGE), :]
                        osend[slot, MERGE * a + b, i * half:(i + 1) * half, :] = part.astype(jnp.bfloat16)
            outward(slot, mate).start()

            @pl.when(inner)
            def _():
                outward(slot, far_low).start()

            @pl.when(jnp.logical_not(inner))
            def _():
                outward(slot, far_low).start()

            outward_own(slot).start()

    @pl.when(inner)
    def _():
        for peer in (far_high,):
            @pl.loop(0, slots)
            def _(slot):
                @pl.when(has(me, slot))
                def _():
                    outward(slot, peer).start()

    @pl.when(jnp.logical_not(inner))
    def _():
        for peer in (far_high,):
            @pl.loop(0, slots)
            def _(slot):
                @pl.when(has(me, slot))
                def _():
                    outward(slot, peer).start()

    wait_bytes(out_ref, merged)
    for _ in range(3):
        wait_bytes(q_ref, sent)


def on_device(queries, key_rows, value_rows):
    n = lax.axis_size("seq")
    if n != MERGE * MERGE:
        return split_features(queries, key_rows, value_rows)
    rows, width = queries.shape
    heads = width // HEAD_DIM
    slots = -(-heads // n)
    total_rows = rows * n
    merged_rows = total_rows // (MERGE * MERGE)
    anywhere = pl.BlockSpec(memory_space=pl.ANY)
    return pl.pallas_call(
        functools.partial(head_kernel, n, heads, math.gcd(total_rows, 256)),
        out_shape=pltpu.VMEM((merged_rows, width), jnp.bfloat16),
        in_specs=[anywhere] * 3,
        out_specs=pl.BlockSpec(memory_space=pltpu.VMEM),
        scratch_shapes=[
            pltpu.VMEM((slots, 3 * total_rows, HEAD_DIM), jnp.bfloat16),
            pltpu.VMEM((total_rows + 8, HEAD_DIM), jnp.float32),
            pltpu.VMEM((slots, n, merged_rows, HEAD_DIM), jnp.bfloat16),
            pltpu.SemaphoreType.DMA((slots,)),
            pltpu.SemaphoreType.DMA,
            pltpu.SemaphoreType.DMA,
            pltpu.SemaphoreType.REGULAR,
            pltpu.SemaphoreType.REGULAR,
            pltpu.SemaphoreType.REGULAR,
        ],
        compiler_params=pltpu.CompilerParams(collective_id=0, has_side_effects=True),
        name="heads_exchange",
    )(queries, key_rows, value_rows)


def solution(mesh):
    placed = (P(("dp", "seq"), None), P(("dp", "seq"), None), P(("dp", "seq"), None))
    return jax.shard_map(
        on_device, mesh=mesh, in_specs=placed, out_specs=P("dp", "seq"), check_vma=False
    )
```

```python
import functools
import math

import jax
import jax.numpy as jnp
from jax import lax
from jax.experimental import pallas as pl
from jax.experimental.pallas import tpu as pltpu
from jax.sharding import PartitionSpec as P

HEAD_DIM = 128
GRID_W = 64
MERGE = 2


def by_heads(queries, key_rows, value_rows, score_scale):
    tok_rows, width = queries.shape
    heads = width // HEAD_DIM
    groups = lax.axis_size("seq")
    padded_heads = -(-heads // groups) * groups

    def spread(source):
        shaped = source.reshape(tok_rows, heads, HEAD_DIM)
        shaped = jnp.pad(shaped, ((0, 0), (0, padded_heads - heads), (0, 0)))
        return shaped.reshape(tok_rows, groups, padded_heads // groups, HEAD_DIM)

    head_query = lax.all_to_all(spread(queries), "seq", split_axis=1, concat_axis=0, tiled=True)
    head_key = lax.all_to_all(spread(key_rows), "seq", split_axis=1, concat_axis=0, tiled=True)
    head_value = lax.all_to_all(spread(value_rows), "seq", split_axis=1, concat_axis=0, tiled=True)
    total_rows = head_query.shape[0]
    head_count = head_query.shape[2]
    flat_key = head_key.reshape(total_rows, head_count, HEAD_DIM)
    flat_value = head_value.reshape(total_rows, head_count, HEAD_DIM)
    step_rows = math.gcd(total_rows, 512)
    blocks = head_query.reshape(total_rows // step_rows, step_rows, head_count, HEAD_DIM)

    def one_block(query_block):
        scores = (
            jnp.einsum("qhd,khd->hqk", query_block, flat_key, preferred_element_type=jnp.float32)
            * score_scale
        )
        row_max = jnp.max(scores, axis=-1, keepdims=True)
        weights = jnp.exp(scores - row_max)
        totals = jnp.sum(weights, axis=-1, keepdims=True)
        weighted = jnp.einsum(
            "hqk,khd->qhd",
            weights.astype(jnp.bfloat16),
            flat_value,
            preferred_element_type=jnp.float32,
        )
        return (weighted / totals.transpose(1, 0, 2)).astype(jnp.bfloat16)

    result = lax.map(one_block, blocks).reshape(total_rows, 1, head_count, HEAD_DIM)
    result = lax.all_to_all(result, "seq", split_axis=0, concat_axis=1, tiled=True)
    return result.reshape(tok_rows, padded_heads, HEAD_DIM)[:, :heads].reshape(tok_rows, width)


def split_features(queries, key_rows, value_rows):
    score_scale = 1.0 / math.sqrt(HEAD_DIM)
    attended = by_heads(queries, key_rows, value_rows, score_scale)
    tok_rows, width = attended.shape
    grid_rows = tok_rows // GRID_W
    shuffled = attended.reshape(grid_rows // 2, 2, GRID_W // 2, 2, width).transpose(0, 2, 1, 3, 4)
    shuffled = shuffled.reshape(grid_rows // 2 * (GRID_W // 2), 4 * width)
    return lax.all_to_all(shuffled, "seq", split_axis=1, concat_axis=0, tiled=True)


def head_kernel(
    n, heads, query_rows,
    q_ref, k_ref, v_ref, out_ref,
    held, obuf, osend, staged,
    loaded, landed, sent, merged, ready, far,
):
    me = lax.axis_index("seq")
    flip = lax.rem(lax.axis_index("dp"), 2)
    base, extra = heads // n, heads % n
    lead = 1 if extra else 0
    slots = base + lead
    rows = q_ref.shape[0]
    total_rows = rows * n
    score_scale = 1.0 / math.sqrt(HEAD_DIM)

    def place(device):
        at = device + 1 - 2 * lax.rem(device, 2)
        return flip * (n - 1 - at) + (1 - flip) * at

    def head_of(device, slot):
        at = place(device)
        regular = at * base + slot - lead
        if not lead:
            return regular
        return jnp.where(slot == 0, n * base + at, regular)

    def has(device, slot):
        if not lead:
            return slot >= 0
        return jnp.logical_or(slot > 0, place(device) < extra)

    def columns(head):
        return pl.ds(pl.multiple_of(head * HEAD_DIM, HEAD_DIM), HEAD_DIM)

    def rows_of(tensor, device):
        return pl.ds(pl.multiple_of(tensor * total_rows + device * rows, rows), rows)

    peers = (n - 1 - me, lax.rem(me + n // 2, n), me + 1 - 2 * lax.rem(me, 2))
    tensors = (k_ref, q_ref, v_ref)

    def inward(t, slot, peer, source=None):
        return pltpu.make_async_remote_copy(
            src_ref=tensors[t].at[:, columns(head_of(peer, slot))] if source is None else source,
            dst_ref=held.at[slot, rows_of(t, me), :],
            send_sem=sent,
            recv_sem=landed.at[slot],
            device_id={"seq": peer},
            device_id_type=pl.DeviceIdType.MESH,
        )

    def inward_own(t, slot):
        return pltpu.make_async_copy(
            tensors[t].at[:, columns(head_of(me, slot))],
            held.at[slot, rows_of(t, me), :],
            landed.at[slot],
        )

    def outward(slot, peer):
        return pltpu.make_async_remote_copy(
            src_ref=osend.at[slot, peer],
            dst_ref=out_ref.at[:, columns(head_of(me, slot))],
            send_sem=sent,
            recv_sem=merged,
            device_id={"seq": peer},
            device_id_type=pl.DeviceIdType.MESH,
        )

    def outward_own(slot):
        return pltpu.make_async_copy(
            osend.at[slot, me], out_ref.at[:, columns(head_of(me, slot))], merged
        )

    def wait_bytes(ref, sem):
        pltpu.make_async_copy(ref, ref, sem).wait()

    partner, across, mate = peers
    far_low = jnp.where(me < n // 2, n // 2, 0)
    far_high = far_low + 1
    inner = (me > 0) & (me < n - 1)
    early = lead + 1

    def tell(sem, device):
        pl.semaphore_signal(
            sem, inc=1, device_id={"seq": device}, device_id_type=pl.DeviceIdType.MESH
        )

    barrier = pltpu.get_barrier_semaphore()

    @pl.when(inner)
    def _():
        tell(barrier, partner)
        tell(barrier, mate)

    left = me == n // 2 - 1

    @pl.when(left)
    def _():
        for t in range(3):
            pltpu.make_async_copy(
                tensors[t].at[:, columns(head_of(partner, lead))], staged.at[t], loaded
            ).start()

    pl.semaphore_wait(barrier, 1)

    @pl.when(inner)
    def _():
        @pl.when(left)
        def _():
            wait_bytes(staged, loaded)
            for t in range(3):
                inward(t, lead, partner, staged.at[t]).start()

        @pl.when(jnp.logical_not(left))
        def _():
            for t in range(3):
                inward(t, lead, partner).start()

        for slot in range(lead):
            for t in range(3):
                @pl.when(has(partner, slot))
                def _():
                    inward(t, slot, partner).start()
        pl.semaphore_wait(ready, 1)
        tell(far, partner)
        pl.semaphore_wait(far, 1)
        tell(far, mate)

    @pl.when(jnp.logical_not(inner))
    def _():
        tell(ready, mate)
        pl.semaphore_wait(far, 1)

    @pl.loop(0, slots)
    def _(slot):
        for t in range(3):
            for peer in peers:
                fresh = has(peer, slot)
                if peer is partner:
                    fresh = fresh & ((slot >= early) | jnp.logical_not(inner))

                @pl.when(fresh)
                def _():
                    inward(t, slot, peer).start()

            @pl.when(has(me, slot))
            def _():
                inward_own(t, slot).start()

    @pl.loop(0, slots)
    def _(slot):
        @pl.when(has(me, slot))
        def _():
            wait_bytes(held.at[slot], landed.at[slot])

            @pl.loop(0, total_rows // query_rows)
            def _(block):
                at = pl.ds(pl.multiple_of(block * query_rows, query_rows), query_rows)
                from_q = pl.ds(pl.multiple_of(total_rows + block * query_rows, query_rows), query_rows)
                scores = lax.dot_general(
                    held[slot, from_q, :], held[slot, pl.ds(0, total_rows), :], (((1,), (1,)), ((), ())),
                    preferred_element_type=jnp.float32,
                ) * score_scale
                row_max = jnp.max(scores, axis=-1, keepdims=True)
                weights = jnp.exp(scores - row_max)
                totals = jnp.sum(weights, axis=-1, keepdims=True)
                weighted = jnp.dot(
                    weights.astype(jnp.bfloat16), held[slot, pl.ds(2 * total_rows, total_rows), :],
                    preferred_element_type=jnp.float32,
                )
                obuf[at, :] = weighted / totals

            half = GRID_W // MERGE
            for a in range(MERGE):
                for b in range(MERGE):
                    for i in range(total_rows // GRID_W // MERGE):
                        part = obuf[pl.ds((MERGE * i + a) * GRID_W + b, half, stride=MERGE), :]
                        osend[slot, MERGE * a + b, i * half:(i + 1) * half, :] = part.astype(jnp.bfloat16)
            outward(slot, mate).start()

            @pl.when(inner)
            def _():
                outward(slot, far_low).start()

            @pl.when(jnp.logical_not(inner))
            def _():
                outward(slot, far_low).start()

            outward_own(slot).start()

    @pl.when(inner)
    def _():
        for peer in (far_high,):
            @pl.loop(0, slots)
            def _(slot):
                @pl.when(has(me, slot))
                def _():
                    outward(slot, peer).start()

    @pl.when(jnp.logical_not(inner))
    def _():
        for peer in (far_high,):
            @pl.loop(0, slots)
            def _(slot):
                @pl.when(has(me, slot))
                def _():
                    outward(slot, peer).start()

    wait_bytes(out_ref, merged)
    for _ in range(3):
        wait_bytes(q_ref, sent)


def on_device(queries, key_rows, value_rows):
    n = lax.axis_size("seq")
    if n != MERGE * MERGE:
        return split_features(queries, key_rows, value_rows)
    rows, width = queries.shape
    heads = width // HEAD_DIM
    slots = -(-heads // n)
    total_rows = rows * n
    merged_rows = total_rows // (MERGE * MERGE)
    anywhere = pl.BlockSpec(memory_space=pl.ANY)
    return pl.pallas_call(
        functools.partial(head_kernel, n, heads, math.gcd(total_rows, 256)),
        out_shape=pltpu.VMEM((merged_rows, width), jnp.bfloat16),
        in_specs=[anywhere] * 3,
        out_specs=pl.BlockSpec(memory_space=pltpu.VMEM),
        scratch_shapes=[
            pltpu.VMEM((slots, 3 * total_rows, HEAD_DIM), jnp.bfloat16),
            pltpu.VMEM((total_rows + 8, HEAD_DIM), jnp.float32),
            pltpu.VMEM((slots, n, merged_rows, HEAD_DIM), jnp.bfloat16),
            pltpu.VMEM((3, rows, HEAD_DIM), jnp.bfloat16),
            pltpu.SemaphoreType.DMA,
            pltpu.SemaphoreType.DMA((slots,)),
            pltpu.SemaphoreType.DMA,
            pltpu.SemaphoreType.DMA,
            pltpu.SemaphoreType.REGULAR,
            pltpu.SemaphoreType.REGULAR,
        ],
        compiler_params=pltpu.CompilerParams(collective_id=0, has_side_effects=True),
        name="heads_exchange",
    )(queries, key_rows, value_rows)


def solution(mesh):
    placed = (P(("dp", "seq"), None), P(("dp", "seq"), None), P(("dp", "seq"), None))
    return jax.shard_map(
        on_device, mesh=mesh, in_specs=placed, out_specs=P("dp", "seq"), check_vma=False
    )
```

```python
import functools
import math

import jax
import jax.numpy as jnp
from jax import lax
from jax.experimental import pallas as pl
from jax.experimental.pallas import tpu as pltpu
from jax.sharding import PartitionSpec as P

HEAD_DIM = 128
GRID_W = 64
MERGE = 2


def by_heads(queries, key_rows, value_rows, score_scale):
    tok_rows, width = queries.shape
    heads = width // HEAD_DIM
    groups = lax.axis_size("seq")
    padded_heads = -(-heads // groups) * groups

    def spread(source):
        shaped = source.reshape(tok_rows, heads, HEAD_DIM)
        shaped = jnp.pad(shaped, ((0, 0), (0, padded_heads - heads), (0, 0)))
        return shaped.reshape(tok_rows, groups, padded_heads // groups, HEAD_DIM)

    head_query = lax.all_to_all(spread(queries), "seq", split_axis=1, concat_axis=0, tiled=True)
    head_key = lax.all_to_all(spread(key_rows), "seq", split_axis=1, concat_axis=0, tiled=True)
    head_value = lax.all_to_all(spread(value_rows), "seq", split_axis=1, concat_axis=0, tiled=True)
    total_rows = head_query.shape[0]
    head_count = head_query.shape[2]
    flat_key = head_key.reshape(total_rows, head_count, HEAD_DIM)
    flat_value = head_value.reshape(total_rows, head_count, HEAD_DIM)
    step_rows = math.gcd(total_rows, 512)
    blocks = head_query.reshape(total_rows // step_rows, step_rows, head_count, HEAD_DIM)

    def one_block(query_block):
        scores = (
            jnp.einsum("qhd,khd->hqk", query_block, flat_key, preferred_element_type=jnp.float32)
            * score_scale
        )
        row_max = jnp.max(scores, axis=-1, keepdims=True)
        weights = jnp.exp(scores - row_max)
        totals = jnp.sum(weights, axis=-1, keepdims=True)
        weighted = jnp.einsum(
            "hqk,khd->qhd",
            weights.astype(jnp.bfloat16),
            flat_value,
            preferred_element_type=jnp.float32,
        )
        return (weighted / totals.transpose(1, 0, 2)).astype(jnp.bfloat16)

    result = lax.map(one_block, blocks).reshape(total_rows, 1, head_count, HEAD_DIM)
    result = lax.all_to_all(result, "seq", split_axis=0, concat_axis=1, tiled=True)
    return result.reshape(tok_rows, padded_heads, HEAD_DIM)[:, :heads].reshape(tok_rows, width)


def split_features(queries, key_rows, value_rows):
    score_scale = 1.0 / math.sqrt(HEAD_DIM)
    attended = by_heads(queries, key_rows, value_rows, score_scale)
    tok_rows, width = attended.shape
    grid_rows = tok_rows // GRID_W
    shuffled = attended.reshape(grid_rows // 2, 2, GRID_W // 2, 2, width).transpose(0, 2, 1, 3, 4)
    shuffled = shuffled.reshape(grid_rows // 2 * (GRID_W // 2), 4 * width)
    return lax.all_to_all(shuffled, "seq", split_axis=1, concat_axis=0, tiled=True)


def head_kernel(
    n, heads, query_rows,
    q_ref, k_ref, v_ref, out_ref,
    held, obuf, osend, staged,
    loaded, landed, sent, merged, ready, far,
):
    me = lax.axis_index("seq")
    flip = lax.rem(lax.axis_index("dp"), 2)
    base, extra = heads // n, heads % n
    lead = 1 if extra else 0
    slots = base + lead
    rows = q_ref.shape[0]
    total_rows = rows * n
    score_scale = 1.0 / math.sqrt(HEAD_DIM)

    def place(device):
        at = device + 1 - 2 * lax.rem(device, 2)
        return flip * (n - 1 - at) + (1 - flip) * at

    def head_of(device, slot):
        at = place(device)
        regular = at * base + slot - lead
        if not lead:
            return regular
        return jnp.where(slot == 0, n * base + at, regular)

    def has(device, slot):
        if not lead:
            return slot >= 0
        return jnp.logical_or(slot > 0, place(device) < extra)

    def columns(head):
        return pl.ds(pl.multiple_of(head * HEAD_DIM, HEAD_DIM), HEAD_DIM)

    def rows_of(tensor, device):
        return pl.ds(pl.multiple_of(tensor * total_rows + device * rows, rows), rows)

    peers = (n - 1 - me, lax.rem(me + n // 2, n), me + 1 - 2 * lax.rem(me, 2))
    tensors = (k_ref, q_ref, v_ref)

    def group_of(slot):
        return slot - jnp.where(slot >= lead, lead, 0)

    def inward(t, slot, peer, source=None):
        return pltpu.make_async_remote_copy(
            src_ref=tensors[t].at[:, columns(head_of(peer, slot))] if source is None else source,
            dst_ref=held.at[slot, rows_of(t, me), :],
            send_sem=sent,
            recv_sem=landed.at[group_of(slot)],
            device_id={"seq": peer},
            device_id_type=pl.DeviceIdType.MESH,
        )

    def inward_own(t, slot):
        return pltpu.make_async_copy(
            tensors[t].at[:, columns(head_of(me, slot))],
            held.at[slot, rows_of(t, me), :],
            landed.at[group_of(slot)],
        )

    def outward(slot, peer):
        return pltpu.make_async_remote_copy(
            src_ref=osend.at[slot, peer],
            dst_ref=out_ref.at[:, columns(head_of(me, slot))],
            send_sem=sent,
            recv_sem=merged,
            device_id={"seq": peer},
            device_id_type=pl.DeviceIdType.MESH,
        )

    def outward_own(slot):
        return pltpu.make_async_copy(
            osend.at[slot, me], out_ref.at[:, columns(head_of(me, slot))], merged
        )

    def wait_bytes(ref, sem):
        pltpu.make_async_copy(ref, ref, sem).wait()

    partner, across, mate = peers
    far_low = jnp.where(me < n // 2, n // 2, 0)
    far_high = far_low + 1
    inner = (me > 0) & (me < n - 1)
    early = lead + 1

    def tell(sem, device):
        pl.semaphore_signal(
            sem, inc=1, device_id={"seq": device}, device_id_type=pl.DeviceIdType.MESH
        )

    barrier = pltpu.get_barrier_semaphore()

    @pl.when(inner)
    def _():
        tell(barrier, partner)
        tell(barrier, mate)

    left = me == n // 2 - 1

    @pl.when(left)
    def _():
        for t in range(3):
            pltpu.make_async_copy(
                tensors[t].at[:, columns(head_of(partner, lead))], staged.at[t], loaded
            ).start()

    pl.semaphore_wait(barrier, 1)

    @pl.when(inner)
    def _():
        @pl.when(left)
        def _():
            wait_bytes(staged, loaded)
            for t in range(3):
                inward(t, lead, partner, staged.at[t]).start()

        @pl.when(jnp.logical_not(left))
        def _():
            for t in range(3):
                inward(t, lead, partner).start()

        for slot in range(lead):
            for t in range(3):
                @pl.when(has(partner, slot))
                def _():
                    inward(t, slot, partner).start()
        pl.semaphore_wait(ready, 1)
        tell(far, partner)
        pl.semaphore_wait(far, 1)
        tell(far, mate)

    @pl.when(jnp.logical_not(inner))
    def _():
        tell(ready, mate)
        pl.semaphore_wait(far, 1)

    @pl.loop(0, slots)
    def _(slot):
        for t in range(3):
            for peer in peers:
                fresh = has(peer, slot)
                if peer is partner:
                    fresh = fresh & ((slot >= early) | jnp.logical_not(inner))

                @pl.when(fresh)
                def _():
                    inward(t, slot, peer).start()

            @pl.when(has(me, slot))
            def _():
                inward_own(t, slot).start()

    @pl.loop(0, slots)
    def _(slot):
        @pl.when(has(me, slot))
        def _():
            first = has(me, 0) if lead else False

            @pl.when((slot == 0) & first)
            def _():
                wait_bytes(held.at[pl.ds(0, early)], landed.at[0])

            @pl.when((slot == lead) & jnp.logical_not(first))
            def _():
                wait_bytes(held.at[lead], landed.at[0])

            @pl.when(slot > lead)
            def _():
                wait_bytes(held.at[slot], landed.at[group_of(slot)])

            @pl.loop(0, total_rows // query_rows)
            def _(block):
                at = pl.ds(pl.multiple_of(block * query_rows, query_rows), query_rows)
                from_q = pl.ds(pl.multiple_of(total_rows + block * query_rows, query_rows), query_rows)
                scores = lax.dot_general(
                    held[slot, from_q, :], held[slot, pl.ds(0, total_rows), :], (((1,), (1,)), ((), ())),
                    preferred_element_type=jnp.float32,
                ) * score_scale
                row_max = jnp.max(scores, axis=-1, keepdims=True)
                weights = jnp.exp(scores - row_max)
                totals = jnp.sum(weights, axis=-1, keepdims=True)
                weighted = jnp.dot(
                    weights.astype(jnp.bfloat16), held[slot, pl.ds(2 * total_rows, total_rows), :],
                    preferred_element_type=jnp.float32,
                )
                obuf[at, :] = weighted / totals

            half = GRID_W // MERGE
            for a in range(MERGE):
                for b in range(MERGE):
                    for i in range(total_rows // GRID_W // MERGE):
                        part = obuf[pl.ds((MERGE * i + a) * GRID_W + b, half, stride=MERGE), :]
                        osend[slot, MERGE * a + b, i * half:(i + 1) * half, :] = part.astype(jnp.bfloat16)
            outward(slot, mate).start()

            @pl.when(inner)
            def _():
                outward(slot, far_low).start()

            @pl.when(jnp.logical_not(inner))
            def _():
                outward(slot, far_low).start()

            outward_own(slot).start()

    @pl.when(inner)
    def _():
        for peer in (far_high,):
            @pl.loop(0, slots)
            def _(slot):
                @pl.when(has(me, slot))
                def _():
                    outward(slot, peer).start()

    @pl.when(jnp.logical_not(inner))
    def _():
        for peer in (far_high,):
            @pl.loop(0, slots)
            def _(slot):
                @pl.when(has(me, slot))
                def _():
                    outward(slot, peer).start()

    for _ in range(3):
        wait_bytes(q_ref, sent)
    wait_bytes(out_ref, merged)


def on_device(queries, key_rows, value_rows):
    n = lax.axis_size("seq")
    if n != MERGE * MERGE:
        return split_features(queries, key_rows, value_rows)
    rows, width = queries.shape
    heads = width // HEAD_DIM
    slots = -(-heads // n)
    total_rows = rows * n
    merged_rows = total_rows // (MERGE * MERGE)
    anywhere = pl.BlockSpec(memory_space=pl.ANY)
    return pl.pallas_call(
        functools.partial(head_kernel, n, heads, math.gcd(total_rows, 256)),
        out_shape=pltpu.VMEM((merged_rows, width), jnp.bfloat16),
        in_specs=[anywhere] * 3,
        out_specs=pl.BlockSpec(memory_space=pltpu.VMEM),
        scratch_shapes=[
            pltpu.VMEM((slots, 3 * total_rows, HEAD_DIM), jnp.bfloat16),
            pltpu.VMEM((total_rows + 8, HEAD_DIM), jnp.float32),
            pltpu.VMEM((slots, n, merged_rows, HEAD_DIM), jnp.bfloat16),
            pltpu.VMEM((3, rows, HEAD_DIM), jnp.bfloat16),
            pltpu.SemaphoreType.DMA,
            pltpu.SemaphoreType.DMA((heads // n,)),
            pltpu.SemaphoreType.DMA,
            pltpu.SemaphoreType.DMA,
            pltpu.SemaphoreType.REGULAR,
            pltpu.SemaphoreType.REGULAR,
        ],
        compiler_params=pltpu.CompilerParams(collective_id=0, has_side_effects=True),
        name="heads_exchange",
    )(queries, key_rows, value_rows)


def solution(mesh):
    placed = (P(("dp", "seq"), None), P(("dp", "seq"), None), P(("dp", "seq"), None))
    return jax.shard_map(
        on_device, mesh=mesh, in_specs=placed, out_specs=P("dp", "seq"), check_vma=False
    )
```

```python
import functools
import math

import jax
import jax.numpy as jnp
from jax import lax
from jax.experimental import pallas as pl
from jax.experimental.pallas import tpu as pltpu
from jax.sharding import PartitionSpec as P

HEAD_DIM = 128
GRID_W = 64
MERGE = 2


def by_heads(queries, key_rows, value_rows, score_scale):
    tok_rows, width = queries.shape
    heads = width // HEAD_DIM
    groups = lax.axis_size("seq")
    padded_heads = -(-heads // groups) * groups

    def spread(source):
        shaped = source.reshape(tok_rows, heads, HEAD_DIM)
        shaped = jnp.pad(shaped, ((0, 0), (0, padded_heads - heads), (0, 0)))
        return shaped.reshape(tok_rows, groups, padded_heads // groups, HEAD_DIM)

    head_query = lax.all_to_all(spread(queries), "seq", split_axis=1, concat_axis=0, tiled=True)
    head_key = lax.all_to_all(spread(key_rows), "seq", split_axis=1, concat_axis=0, tiled=True)
    head_value = lax.all_to_all(spread(value_rows), "seq", split_axis=1, concat_axis=0, tiled=True)
    total_rows = head_query.shape[0]
    head_count = head_query.shape[2]
    flat_key = head_key.reshape(total_rows, head_count, HEAD_DIM)
    flat_value = head_value.reshape(total_rows, head_count, HEAD_DIM)
    step_rows = math.gcd(total_rows, 512)
    blocks = head_query.reshape(total_rows // step_rows, step_rows, head_count, HEAD_DIM)

    def one_block(query_block):
        scores = (
            jnp.einsum("qhd,khd->hqk", query_block, flat_key, preferred_element_type=jnp.float32)
            * score_scale
        )
        row_max = jnp.max(scores, axis=-1, keepdims=True)
        weights = jnp.exp(scores - row_max)
        totals = jnp.sum(weights, axis=-1, keepdims=True)
        weighted = jnp.einsum(
            "hqk,khd->qhd",
            weights.astype(jnp.bfloat16),
            flat_value,
            preferred_element_type=jnp.float32,
        )
        return (weighted / totals.transpose(1, 0, 2)).astype(jnp.bfloat16)

    result = lax.map(one_block, blocks).reshape(total_rows, 1, head_count, HEAD_DIM)
    result = lax.all_to_all(result, "seq", split_axis=0, concat_axis=1, tiled=True)
    return result.reshape(tok_rows, padded_heads, HEAD_DIM)[:, :heads].reshape(tok_rows, width)


def split_features(queries, key_rows, value_rows):
    score_scale = 1.0 / math.sqrt(HEAD_DIM)
    attended = by_heads(queries, key_rows, value_rows, score_scale)
    tok_rows, width = attended.shape
    grid_rows = tok_rows // GRID_W
    shuffled = attended.reshape(grid_rows // 2, 2, GRID_W // 2, 2, width).transpose(0, 2, 1, 3, 4)
    shuffled = shuffled.reshape(grid_rows // 2 * (GRID_W // 2), 4 * width)
    return lax.all_to_all(shuffled, "seq", split_axis=1, concat_axis=0, tiled=True)


def head_kernel(
    n, heads, query_rows,
    q_ref, k_ref, v_ref, out_ref,
    held, obuf, osend, staged,
    loaded, landed, sent, merged, ready, far,
):
    me = lax.axis_index("seq")
    flip = lax.rem(lax.axis_index("dp"), 2)
    base, extra = heads // n, heads % n
    lead = 1 if extra else 0
    slots = base + lead
    rows = q_ref.shape[0]
    total_rows = rows * n
    score_scale = 1.0 / math.sqrt(HEAD_DIM)

    def place(device):
        at = device + 1 - 2 * lax.rem(device, 2)
        return flip * (n - 1 - at) + (1 - flip) * at

    def head_of(device, slot):
        at = place(device)
        regular = at * base + slot - lead
        if not lead:
            return regular
        return jnp.where(slot == 0, n * base + at, regular)

    def has(device, slot):
        if not lead:
            return slot >= 0
        return jnp.logical_or(slot > 0, place(device) < extra)

    def columns(head):
        return pl.ds(pl.multiple_of(head * HEAD_DIM, HEAD_DIM), HEAD_DIM)

    def rows_of(tensor, device):
        return pl.ds(pl.multiple_of(tensor * total_rows + device * rows, rows), rows)

    peers = (n - 1 - me, lax.rem(me + n // 2, n), me + 1 - 2 * lax.rem(me, 2))
    tensors = (k_ref, q_ref, v_ref)

    def group_of(slot):
        return slot - jnp.where(slot >= lead, lead, 0)

    def inward(t, slot, peer, source=None):
        return pltpu.make_async_remote_copy(
            src_ref=tensors[t].at[:, columns(head_of(peer, slot))] if source is None else source,
            dst_ref=held.at[slot, rows_of(t, me), :],
            send_sem=sent,
            recv_sem=landed.at[group_of(slot)],
            device_id={"seq": peer},
            device_id_type=pl.DeviceIdType.MESH,
        )

    def inward_own(t, slot):
        return pltpu.make_async_copy(
            tensors[t].at[:, columns(head_of(me, slot))],
            held.at[slot, rows_of(t, me), :],
            landed.at[group_of(slot)],
        )

    def outward(slot, peer):
        return pltpu.make_async_remote_copy(
            src_ref=osend.at[slot, peer],
            dst_ref=out_ref.at[:, columns(head_of(me, slot))],
            send_sem=sent,
            recv_sem=merged,
            device_id={"seq": peer},
            device_id_type=pl.DeviceIdType.MESH,
        )

    def outward_own(slot):
        return pltpu.make_async_copy(
            osend.at[slot, me], out_ref.at[:, columns(head_of(me, slot))], merged
        )

    def wait_bytes(ref, sem):
        pltpu.make_async_copy(ref, ref, sem).wait()

    partner, across, mate = peers
    far_low = jnp.where(me < n // 2, n // 2, 0)
    far_high = far_low + 1
    inner = (me > 0) & (me < n - 1)
    early = lead + 1

    def tell(sem, device):
        pl.semaphore_signal(
            sem, inc=1, device_id={"seq": device}, device_id_type=pl.DeviceIdType.MESH
        )

    barrier = pltpu.get_barrier_semaphore()

    @pl.when(inner)
    def _():
        tell(barrier, partner)
        tell(barrier, mate)

    left = me == n // 2 - 1

    @pl.when(left)
    def _():
        for t in range(3):
            pltpu.make_async_copy(
                tensors[t].at[:, columns(head_of(partner, lead))], staged.at[t], loaded
            ).start()

    pl.semaphore_wait(barrier, 1)

    @pl.when(inner)
    def _():
        @pl.when(jnp.logical_not(left))
        def _():
            for t in range(3):
                inward(t, lead, partner).start()

        @pl.when(left)
        def _():
            wait_bytes(staged, loaded)
            for t in range(3):
                inward(t, lead, partner, staged.at[t]).start()

        for slot in range(lead):
            for t in range(3):
                @pl.when(has(partner, slot))
                def _():
                    inward(t, slot, partner).start()
        pl.semaphore_wait(ready, 1)
        tell(far, partner)
        pl.semaphore_wait(far, 1)
        tell(far, mate)

    @pl.when(jnp.logical_not(inner))
    def _():
        tell(ready, mate)
        pl.semaphore_wait(far, 1)

    @pl.loop(0, slots)
    def _(slot):
        for t in range(3):
            for peer in peers:
                fresh = has(peer, slot)
                if peer is partner:
                    fresh = fresh & ((slot >= early) | jnp.logical_not(inner))

                @pl.when(fresh)
                def _():
                    inward(t, slot, peer).start()

            @pl.when(has(me, slot))
            def _():
                inward_own(t, slot).start()

    @pl.loop(0, slots)
    def _(slot):
        @pl.when(has(me, slot))
        def _():
            first = has(me, 0) if lead else False

            @pl.when((slot == 0) & first)
            def _():
                wait_bytes(held.at[pl.ds(0, early)], landed.at[0])

            @pl.when((slot == lead) & jnp.logical_not(first))
            def _():
                wait_bytes(held.at[lead], landed.at[0])

            @pl.when(slot > lead)
            def _():
                wait_bytes(held.at[slot], landed.at[group_of(slot)])

            @pl.loop(0, total_rows // query_rows)
            def _(block):
                at = pl.ds(pl.multiple_of(block * query_rows, query_rows), query_rows)
                from_q = pl.ds(pl.multiple_of(total_rows + block * query_rows, query_rows), query_rows)
                scores = lax.dot_general(
                    held[slot, from_q, :], held[slot, pl.ds(0, total_rows), :], (((1,), (1,)), ((), ())),
                    preferred_element_type=jnp.float32,
                ) * score_scale
                row_max = jnp.max(scores, axis=-1, keepdims=True)
                weights = jnp.exp(scores - row_max)
                totals = jnp.sum(weights, axis=-1, keepdims=True)
                weighted = jnp.dot(
                    weights.astype(jnp.bfloat16), held[slot, pl.ds(2 * total_rows, total_rows), :],
                    preferred_element_type=jnp.float32,
                )
                obuf[at, :] = weighted / totals

            half = GRID_W // MERGE
            for a in range(MERGE):
                for b in range(MERGE):
                    for i in range(total_rows // GRID_W // MERGE):
                        part = obuf[pl.ds((MERGE * i + a) * GRID_W + b, half, stride=MERGE), :]
                        osend[slot, MERGE * a + b, i * half:(i + 1) * half, :] = part.astype(jnp.bfloat16)
            outward(slot, mate).start()

            @pl.when(inner)
            def _():
                outward(slot, far_low).start()

            @pl.when(jnp.logical_not(inner))
            def _():
                outward(slot, far_low).start()

            outward_own(slot).start()

    @pl.when(inner)
    def _():
        for peer in (far_high,):
            @pl.loop(0, slots)
            def _(slot):
                @pl.when(has(me, slot))
                def _():
                    outward(slot, peer).start()

    @pl.when(jnp.logical_not(inner))
    def _():
        for peer in (far_high,):
            @pl.loop(0, slots)
            def _(slot):
                @pl.when(has(me, slot))
                def _():
                    outward(slot, peer).start()

    for _ in range(3):
        wait_bytes(q_ref, sent)
    wait_bytes(out_ref, merged)


def on_device(queries, key_rows, value_rows):
    n = lax.axis_size("seq")
    if n != MERGE * MERGE:
        return split_features(queries, key_rows, value_rows)
    rows, width = queries.shape
    heads = width // HEAD_DIM
    slots = -(-heads // n)
    total_rows = rows * n
    merged_rows = total_rows // (MERGE * MERGE)
    anywhere = pl.BlockSpec(memory_space=pl.ANY)
    return pl.pallas_call(
        functools.partial(head_kernel, n, heads, math.gcd(total_rows, 256)),
        out_shape=pltpu.VMEM((merged_rows, width), jnp.bfloat16),
        in_specs=[anywhere] * 3,
        out_specs=pl.BlockSpec(memory_space=pltpu.VMEM),
        scratch_shapes=[
            pltpu.VMEM((slots, 3 * total_rows, HEAD_DIM), jnp.bfloat16),
            pltpu.VMEM((total_rows + 8, HEAD_DIM), jnp.float32),
            pltpu.VMEM((slots, n, merged_rows, HEAD_DIM), jnp.bfloat16),
            pltpu.VMEM((3, rows, HEAD_DIM), jnp.bfloat16),
            pltpu.SemaphoreType.DMA,
            pltpu.SemaphoreType.DMA((heads // n,)),
            pltpu.SemaphoreType.DMA,
            pltpu.SemaphoreType.DMA,
            pltpu.SemaphoreType.REGULAR,
            pltpu.SemaphoreType.REGULAR,
        ],
        compiler_params=pltpu.CompilerParams(collective_id=0, has_side_effects=True),
        name="heads_exchange",
    )(queries, key_rows, value_rows)


def solution(mesh):
    placed = (P(("dp", "seq"), None), P(("dp", "seq"), None), P(("dp", "seq"), None))
    return jax.shard_map(
        on_device, mesh=mesh, in_specs=placed, out_specs=P("dp", "seq"), check_vma=False
    )
```

```python
import functools
import math

import jax
import jax.numpy as jnp
from jax import lax
from jax.experimental import pallas as pl
from jax.experimental.pallas import tpu as pltpu
from jax.sharding import PartitionSpec as P

HEAD_DIM = 128
GRID_W = 64
MERGE = 2


def by_heads(queries, key_rows, value_rows, score_scale):
    tok_rows, width = queries.shape
    heads = width // HEAD_DIM
    groups = lax.axis_size("seq")
    padded_heads = -(-heads // groups) * groups

    def spread(source):
        shaped = source.reshape(tok_rows, heads, HEAD_DIM)
        shaped = jnp.pad(shaped, ((0, 0), (0, padded_heads - heads), (0, 0)))
        return shaped.reshape(tok_rows, groups, padded_heads // groups, HEAD_DIM)

    head_query = lax.all_to_all(spread(queries), "seq", split_axis=1, concat_axis=0, tiled=True)
    head_key = lax.all_to_all(spread(key_rows), "seq", split_axis=1, concat_axis=0, tiled=True)
    head_value = lax.all_to_all(spread(value_rows), "seq", split_axis=1, concat_axis=0, tiled=True)
    total_rows = head_query.shape[0]
    head_count = head_query.shape[2]
    flat_key = head_key.reshape(total_rows, head_count, HEAD_DIM)
    flat_value = head_value.reshape(total_rows, head_count, HEAD_DIM)
    step_rows = math.gcd(total_rows, 512)
    blocks = head_query.reshape(total_rows // step_rows, step_rows, head_count, HEAD_DIM)

    def one_block(query_block):
        scores = (
            jnp.einsum("qhd,khd->hqk", query_block, flat_key, preferred_element_type=jnp.float32)
            * score_scale
        )
        row_max = jnp.max(scores, axis=-1, keepdims=True)
        weights = jnp.exp(scores - row_max)
        totals = jnp.sum(weights, axis=-1, keepdims=True)
        weighted = jnp.einsum(
            "hqk,khd->qhd",
            weights.astype(jnp.bfloat16),
            flat_value,
            preferred_element_type=jnp.float32,
        )
        return (weighted / totals.transpose(1, 0, 2)).astype(jnp.bfloat16)

    result = lax.map(one_block, blocks).reshape(total_rows, 1, head_count, HEAD_DIM)
    result = lax.all_to_all(result, "seq", split_axis=0, concat_axis=1, tiled=True)
    return result.reshape(tok_rows, padded_heads, HEAD_DIM)[:, :heads].reshape(tok_rows, width)


def split_features(queries, key_rows, value_rows):
    score_scale = 1.0 / math.sqrt(HEAD_DIM)
    attended = by_heads(queries, key_rows, value_rows, score_scale)
    tok_rows, width = attended.shape
    grid_rows = tok_rows // GRID_W
    shuffled = attended.reshape(grid_rows // 2, 2, GRID_W // 2, 2, width).transpose(0, 2, 1, 3, 4)
    shuffled = shuffled.reshape(grid_rows // 2 * (GRID_W // 2), 4 * width)
    return lax.all_to_all(shuffled, "seq", split_axis=1, concat_axis=0, tiled=True)


def head_kernel(
    n, heads, query_rows,
    q_ref, k_ref, v_ref, out_ref,
    held, obuf, osend, staged,
    loaded, landed, sent, merged, ready, far,
):
    me = lax.axis_index("seq")
    inner = (me > 0) & (me < n - 1)
    partner = n - 1 - me
    mate = me + jnp.where(inner, 1, -1) * jnp.where(me < n // 2, -1, 1)

    def tell(sem, device):
        pl.semaphore_signal(
            sem, inc=1, device_id={"seq": device}, device_id_type=pl.DeviceIdType.MESH
        )

    barrier = pltpu.get_barrier_semaphore()

    @pl.when(inner)
    def _():
        tell(barrier, partner)
        tell(barrier, mate)

    flip = lax.rem(lax.axis_index("dp"), 2)
    base, extra = heads // n, heads % n
    lead = 1 if extra else 0
    slots = base + lead
    rows = q_ref.shape[0]
    total_rows = rows * n
    score_scale = 1.0 / math.sqrt(HEAD_DIM)

    def place(device):
        at = device + 1 - 2 * lax.rem(device, 2)
        return flip * (n - 1 - at) + (1 - flip) * at

    def head_of(device, slot):
        at = place(device)
        regular = at * base + slot - lead
        if not lead:
            return regular
        return jnp.where(slot == 0, n * base + at, regular)

    def has(device, slot):
        if not lead:
            return slot >= 0
        return jnp.logical_or(slot > 0, place(device) < extra)

    def columns(head):
        return pl.ds(pl.multiple_of(head * HEAD_DIM, HEAD_DIM), HEAD_DIM)

    def rows_of(tensor, device):
        return pl.ds(pl.multiple_of(tensor * total_rows + device * rows, rows), rows)

    across = me + jnp.where(me < n // 2, n // 2, -(n // 2))
    peers = (partner, across, mate)
    tensors = (k_ref, q_ref, v_ref)

    def group_of(slot):
        return slot - jnp.where(slot >= lead, lead, 0)

    def inward(t, slot, peer, source=None):
        return pltpu.make_async_remote_copy(
            src_ref=tensors[t].at[:, columns(head_of(peer, slot))] if source is None else source,
            dst_ref=held.at[slot, rows_of(t, me), :],
            send_sem=sent,
            recv_sem=landed.at[group_of(slot)],
            device_id={"seq": peer},
            device_id_type=pl.DeviceIdType.MESH,
        )

    def inward_own(t, slot):
        return pltpu.make_async_copy(
            tensors[t].at[:, columns(head_of(me, slot))],
            held.at[slot, rows_of(t, me), :],
            landed.at[group_of(slot)],
        )

    def outward(slot, peer):
        return pltpu.make_async_remote_copy(
            src_ref=osend.at[slot, peer],
            dst_ref=out_ref.at[:, columns(head_of(me, slot))],
            send_sem=sent,
            recv_sem=merged,
            device_id={"seq": peer},
            device_id_type=pl.DeviceIdType.MESH,
        )

    def outward_own(slot):
        return pltpu.make_async_copy(
            osend.at[slot, me], out_ref.at[:, columns(head_of(me, slot))], merged
        )

    def wait_bytes(ref, sem):
        pltpu.make_async_copy(ref, ref, sem).wait()

    far_low = jnp.where(me < n // 2, n // 2, 0)
    far_high = far_low + 1
    early = lead + 1

    left = me == n // 2 - 1

    @pl.when(left)
    def _():
        for t in range(3):
            pltpu.make_async_copy(
                tensors[t].at[:, columns(head_of(partner, lead))], staged.at[t], loaded
            ).start()

    pl.semaphore_wait(barrier, 1)

    @pl.when(inner)
    def _():
        @pl.when(jnp.logical_not(left))
        def _():
            for t in range(3):
                inward(t, lead, partner).start()

        @pl.when(left)
        def _():
            wait_bytes(staged, loaded)
            for t in range(3):
                inward(t, lead, partner, staged.at[t]).start()

        for slot in range(lead):
            for t in range(3):
                @pl.when(has(partner, slot))
                def _():
                    inward(t, slot, partner).start()
        pl.semaphore_wait(ready, 1)
        tell(far, partner)
        pl.semaphore_wait(far, 1)
        tell(far, mate)

    @pl.when(jnp.logical_not(inner))
    def _():
        tell(ready, mate)
        pl.semaphore_wait(far, 1)

    @pl.loop(0, slots)
    def _(slot):
        for t in range(3):
            for peer in peers:
                fresh = has(peer, slot)
                if peer is partner:
                    fresh = fresh & ((slot >= early) | jnp.logical_not(inner))

                @pl.when(fresh)
                def _():
                    inward(t, slot, peer).start()

            @pl.when(has(me, slot))
            def _():
                inward_own(t, slot).start()

    @pl.loop(0, slots)
    def _(slot):
        @pl.when(has(me, slot))
        def _():
            first = has(me, 0) if lead else False

            @pl.when((slot == 0) & first)
            def _():
                wait_bytes(held.at[pl.ds(0, early)], landed.at[0])

            @pl.when((slot == lead) & jnp.logical_not(first))
            def _():
                wait_bytes(held.at[lead], landed.at[0])

            @pl.when(slot > lead)
            def _():
                wait_bytes(held.at[slot], landed.at[group_of(slot)])

            @pl.loop(0, total_rows // query_rows)
            def _(block):
                at = pl.ds(pl.multiple_of(block * query_rows, query_rows), query_rows)
                from_q = pl.ds(pl.multiple_of(total_rows + block * query_rows, query_rows), query_rows)
                scores = lax.dot_general(
                    held[slot, from_q, :], held[slot, pl.ds(0, total_rows), :], (((1,), (1,)), ((), ())),
                    preferred_element_type=jnp.float32,
                ) * score_scale
                row_max = jnp.max(scores, axis=-1, keepdims=True)
                weights = jnp.exp(scores - row_max)
                totals = jnp.sum(weights, axis=-1, keepdims=True)
                weighted = jnp.dot(
                    weights.astype(jnp.bfloat16), held[slot, pl.ds(2 * total_rows, total_rows), :],
                    preferred_element_type=jnp.float32,
                )
                obuf[at, :] = weighted / totals

            half = GRID_W // MERGE
            for a in range(MERGE):
                for b in range(MERGE):
                    for i in range(total_rows // GRID_W // MERGE):
                        part = obuf[pl.ds((MERGE * i + a) * GRID_W + b, half, stride=MERGE), :]
                        osend[slot, MERGE * a + b, i * half:(i + 1) * half, :] = part.astype(jnp.bfloat16)
            outward(slot, mate).start()

            @pl.when(inner)
            def _():
                outward(slot, far_low).start()

            @pl.when(jnp.logical_not(inner))
            def _():
                outward(slot, far_low).start()

            outward_own(slot).start()

    @pl.when(inner)
    def _():
        for peer in (far_high,):
            @pl.loop(0, slots)
            def _(slot):
                @pl.when(has(me, slot))
                def _():
                    outward(slot, peer).start()

    @pl.when(jnp.logical_not(inner))
    def _():
        for peer in (far_high,):
            @pl.loop(0, slots)
            def _(slot):
                @pl.when(has(me, slot))
                def _():
                    outward(slot, peer).start()

    for _ in range(3):
        wait_bytes(q_ref, sent)
    wait_bytes(out_ref, merged)


def on_device(queries, key_rows, value_rows):
    n = lax.axis_size("seq")
    if n != MERGE * MERGE:
        return split_features(queries, key_rows, value_rows)
    rows, width = queries.shape
    heads = width // HEAD_DIM
    slots = -(-heads // n)
    total_rows = rows * n
    merged_rows = total_rows // (MERGE * MERGE)
    anywhere = pl.BlockSpec(memory_space=pl.ANY)
    return pl.pallas_call(
        functools.partial(head_kernel, n, heads, math.gcd(total_rows, 256)),
        out_shape=pltpu.VMEM((merged_rows, width), jnp.bfloat16),
        in_specs=[anywhere] * 3,
        out_specs=pl.BlockSpec(memory_space=pltpu.VMEM),
        scratch_shapes=[
            pltpu.VMEM((slots, 3 * total_rows, HEAD_DIM), jnp.bfloat16),
            pltpu.VMEM((total_rows + 8, HEAD_DIM), jnp.float32),
            pltpu.VMEM((slots, n, merged_rows, HEAD_DIM), jnp.bfloat16),
            pltpu.VMEM((3, rows, HEAD_DIM), jnp.bfloat16),
            pltpu.SemaphoreType.DMA,
            pltpu.SemaphoreType.DMA((heads // n,)),
            pltpu.SemaphoreType.DMA,
            pltpu.SemaphoreType.DMA,
            pltpu.SemaphoreType.REGULAR,
            pltpu.SemaphoreType.REGULAR,
        ],
        compiler_params=pltpu.CompilerParams(collective_id=0, has_side_effects=True),
        name="heads_exchange",
    )(queries, key_rows, value_rows)


def solution(mesh):
    placed = (P(("dp", "seq"), None), P(("dp", "seq"), None), P(("dp", "seq"), None))
    return jax.shard_map(
        on_device, mesh=mesh, in_specs=placed, out_specs=P("dp", "seq"), check_vma=False
    )
```

```python
import functools
import math

import jax
import jax.numpy as jnp
from jax import lax
from jax.experimental import pallas as pl
from jax.experimental.pallas import tpu as pltpu
from jax.sharding import PartitionSpec as P

HEAD_DIM = 128
GRID_W = 64
MERGE = 2


def by_heads(queries, key_rows, value_rows, score_scale):
    tok_rows, width = queries.shape
    heads = width // HEAD_DIM
    groups = lax.axis_size("seq")
    padded_heads = -(-heads // groups) * groups

    def spread(source):
        shaped = source.reshape(tok_rows, heads, HEAD_DIM)
        shaped = jnp.pad(shaped, ((0, 0), (0, padded_heads - heads), (0, 0)))
        return shaped.reshape(tok_rows, groups, padded_heads // groups, HEAD_DIM)

    head_query = lax.all_to_all(spread(queries), "seq", split_axis=1, concat_axis=0, tiled=True)
    head_key = lax.all_to_all(spread(key_rows), "seq", split_axis=1, concat_axis=0, tiled=True)
    head_value = lax.all_to_all(spread(value_rows), "seq", split_axis=1, concat_axis=0, tiled=True)
    total_rows = head_query.shape[0]
    head_count = head_query.shape[2]
    flat_key = head_key.reshape(total_rows, head_count, HEAD_DIM)
    flat_value = head_value.reshape(total_rows, head_count, HEAD_DIM)
    step_rows = math.gcd(total_rows, 512)
    blocks = head_query.reshape(total_rows // step_rows, step_rows, head_count, HEAD_DIM)

    def one_block(query_block):
        scores = (
            jnp.einsum("qhd,khd->hqk", query_block, flat_key, preferred_element_type=jnp.float32)
            * score_scale
        )
        row_max = jnp.max(scores, axis=-1, keepdims=True)
        weights = jnp.exp(scores - row_max)
        totals = jnp.sum(weights, axis=-1, keepdims=True)
        weighted = jnp.einsum(
            "hqk,khd->qhd",
            weights.astype(jnp.bfloat16),
            flat_value,
            preferred_element_type=jnp.float32,
        )
        return (weighted / totals.transpose(1, 0, 2)).astype(jnp.bfloat16)

    result = lax.map(one_block, blocks).reshape(total_rows, 1, head_count, HEAD_DIM)
    result = lax.all_to_all(result, "seq", split_axis=0, concat_axis=1, tiled=True)
    return result.reshape(tok_rows, padded_heads, HEAD_DIM)[:, :heads].reshape(tok_rows, width)


def split_features(queries, key_rows, value_rows):
    score_scale = 1.0 / math.sqrt(HEAD_DIM)
    attended = by_heads(queries, key_rows, value_rows, score_scale)
    tok_rows, width = attended.shape
    grid_rows = tok_rows // GRID_W
    shuffled = attended.reshape(grid_rows // 2, 2, GRID_W // 2, 2, width).transpose(0, 2, 1, 3, 4)
    shuffled = shuffled.reshape(grid_rows // 2 * (GRID_W // 2), 4 * width)
    return lax.all_to_all(shuffled, "seq", split_axis=1, concat_axis=0, tiled=True)


def head_kernel(
    n, heads, query_rows,
    q_ref, k_ref, v_ref, out_ref,
    held, obuf, osend, staged,
    loaded, landed, sent, merged, ready, far,
):
    me = lax.axis_index("seq")
    inner = (me > 0) & (me < n - 1)
    partner = n - 1 - me
    mate = me + jnp.where(inner, 1, -1) * jnp.where(me < n // 2, -1, 1)

    def tell(sem, device):
        pl.semaphore_signal(
            sem, inc=1, device_id={"seq": device}, device_id_type=pl.DeviceIdType.MESH
        )

    barrier = pltpu.get_barrier_semaphore()

    @pl.when(inner)
    def _():
        tell(barrier, partner)

    @pl.when(me == n // 2 - 1)
    def _():
        tell(barrier, mate)

    flip = lax.rem(lax.axis_index("dp"), 2)
    base, extra = heads // n, heads % n
    lead = 1 if extra else 0
    slots = base + lead
    rows = q_ref.shape[0]
    total_rows = rows * n
    score_scale = 1.0 / math.sqrt(HEAD_DIM)

    def place(device):
        at = device + 1 - 2 * lax.rem(device, 2)
        return flip * (n - 1 - at) + (1 - flip) * at

    def head_of(device, slot):
        at = place(device)
        regular = at * base + slot - lead
        if not lead:
            return regular
        return jnp.where(slot == 0, n * base + at, regular)

    def has(device, slot):
        if not lead:
            return slot >= 0
        return jnp.logical_or(slot > 0, place(device) < extra)

    def columns(head):
        return pl.ds(pl.multiple_of(head * HEAD_DIM, HEAD_DIM), HEAD_DIM)

    def rows_of(tensor, device):
        return pl.ds(pl.multiple_of(tensor * total_rows + device * rows, rows), rows)

    across = me + jnp.where(me < n // 2, n // 2, -(n // 2))
    peers = (partner, across, mate)
    tensors = (k_ref, q_ref, v_ref)

    def group_of(slot):
        return slot - jnp.where(slot >= lead, lead, 0)

    def inward(t, slot, peer, source=None):
        return pltpu.make_async_remote_copy(
            src_ref=tensors[t].at[:, columns(head_of(peer, slot))] if source is None else source,
            dst_ref=held.at[slot, rows_of(t, me), :],
            send_sem=sent,
            recv_sem=landed.at[group_of(slot)],
            device_id={"seq": peer},
            device_id_type=pl.DeviceIdType.MESH,
        )

    def inward_own(t, slot):
        return pltpu.make_async_copy(
            tensors[t].at[:, columns(head_of(me, slot))],
            held.at[slot, rows_of(t, me), :],
            landed.at[group_of(slot)],
        )

    def outward(slot, peer):
        return pltpu.make_async_remote_copy(
            src_ref=osend.at[slot, peer],
            dst_ref=out_ref.at[:, columns(head_of(me, slot))],
            send_sem=sent,
            recv_sem=merged,
            device_id={"seq": peer},
            device_id_type=pl.DeviceIdType.MESH,
        )

    def outward_own(slot):
        return pltpu.make_async_copy(
            osend.at[slot, me], out_ref.at[:, columns(head_of(me, slot))], merged
        )

    def wait_bytes(ref, sem):
        pltpu.make_async_copy(ref, ref, sem).wait()

    far_low = jnp.where(me < n // 2, n // 2, 0)
    far_high = far_low + 1
    early = lead + 1

    left = me == n // 2 - 1

    @pl.when(left)
    def _():
        for t in range(3):
            pltpu.make_async_copy(
                tensors[t].at[:, columns(head_of(partner, lead))], staged.at[t], loaded
            ).start()

    pl.semaphore_wait(barrier, 1)

    @pl.when(inner)
    def _():
        @pl.when(jnp.logical_not(left))
        def _():
            for t in range(3):
                inward(t, lead, partner).start()
            tell(barrier, mate)

        @pl.when(left)
        def _():
            wait_bytes(staged, loaded)
            for t in range(3):
                inward(t, lead, partner, staged.at[t]).start()

        for slot in range(lead):
            for t in range(3):
                @pl.when(has(partner, slot))
                def _():
                    inward(t, slot, partner).start()
        pl.semaphore_wait(ready, 1)
        tell(far, partner)
        pl.semaphore_wait(far, 1)
        tell(far, mate)

    @pl.when(jnp.logical_not(inner))
    def _():
        tell(ready, mate)
        pl.semaphore_wait(far, 1)

    @pl.loop(0, slots)
    def _(slot):
        for t in range(3):
            for peer in peers:
                fresh = has(peer, slot)
                if peer is partner:
                    fresh = fresh & ((slot >= early) | jnp.logical_not(inner))

                @pl.when(fresh)
                def _():
                    inward(t, slot, peer).start()

            @pl.when(has(me, slot))
            def _():
                inward_own(t, slot).start()

    @pl.loop(0, slots)
    def _(slot):
        @pl.when(has(me, slot))
        def _():
            first = has(me, 0) if lead else False

            @pl.when((slot == 0) & first)
            def _():
                wait_bytes(held.at[pl.ds(0, early)], landed.at[0])

            @pl.when((slot == lead) & jnp.logical_not(first))
            def _():
                wait_bytes(held.at[lead], landed.at[0])

            @pl.when(slot > lead)
            def _():
                wait_bytes(held.at[slot], landed.at[group_of(slot)])

            @pl.loop(0, total_rows // query_rows)
            def _(block):
                at = pl.ds(pl.multiple_of(block * query_rows, query_rows), query_rows)
                from_q = pl.ds(pl.multiple_of(total_rows + block * query_rows, query_rows), query_rows)
                scores = lax.dot_general(
                    held[slot, from_q, :], held[slot, pl.ds(0, total_rows), :], (((1,), (1,)), ((), ())),
                    preferred_element_type=jnp.float32,
                ) * score_scale
                row_max = jnp.max(scores, axis=-1, keepdims=True)
                weights = jnp.exp(scores - row_max)
                totals = jnp.sum(weights, axis=-1, keepdims=True)
                weighted = jnp.dot(
                    weights.astype(jnp.bfloat16), held[slot, pl.ds(2 * total_rows, total_rows), :],
                    preferred_element_type=jnp.float32,
                )
                obuf[at, :] = weighted / totals

            half = GRID_W // MERGE
            for a in range(MERGE):
                for b in range(MERGE):
                    for i in range(total_rows // GRID_W // MERGE):
                        part = obuf[pl.ds((MERGE * i + a) * GRID_W + b, half, stride=MERGE), :]
                        osend[slot, MERGE * a + b, i * half:(i + 1) * half, :] = part.astype(jnp.bfloat16)
            outward(slot, mate).start()

            @pl.when(inner)
            def _():
                outward(slot, far_low).start()

            @pl.when(jnp.logical_not(inner))
            def _():
                outward(slot, far_low).start()

            outward_own(slot).start()

    @pl.when(inner)
    def _():
        for peer in (far_high,):
            @pl.loop(0, slots)
            def _(slot):
                @pl.when(has(me, slot))
                def _():
                    outward(slot, peer).start()

    @pl.when(jnp.logical_not(inner))
    def _():
        for peer in (far_high,):
            @pl.loop(0, slots)
            def _(slot):
                @pl.when(has(me, slot))
                def _():
                    outward(slot, peer).start()

    for _ in range(3):
        wait_bytes(q_ref, sent)
    wait_bytes(out_ref, merged)


def on_device(queries, key_rows, value_rows):
    n = lax.axis_size("seq")
    if n != MERGE * MERGE:
        return split_features(queries, key_rows, value_rows)
    rows, width = queries.shape
    heads = width // HEAD_DIM
    slots = -(-heads // n)
    total_rows = rows * n
    merged_rows = total_rows // (MERGE * MERGE)
    anywhere = pl.BlockSpec(memory_space=pl.ANY)
    return pl.pallas_call(
        functools.partial(head_kernel, n, heads, math.gcd(total_rows, 256)),
        out_shape=pltpu.VMEM((merged_rows, width), jnp.bfloat16),
        in_specs=[anywhere] * 3,
        out_specs=pl.BlockSpec(memory_space=pltpu.VMEM),
        scratch_shapes=[
            pltpu.VMEM((slots, 3 * total_rows, HEAD_DIM), jnp.bfloat16),
            pltpu.VMEM((total_rows + 8, HEAD_DIM), jnp.float32),
            pltpu.VMEM((slots, n, merged_rows, HEAD_DIM), jnp.bfloat16),
            pltpu.VMEM((3, rows, HEAD_DIM), jnp.bfloat16),
            pltpu.SemaphoreType.DMA,
            pltpu.SemaphoreType.DMA((heads // n,)),
            pltpu.SemaphoreType.DMA,
            pltpu.SemaphoreType.DMA,
            pltpu.SemaphoreType.REGULAR,
            pltpu.SemaphoreType.REGULAR,
        ],
        compiler_params=pltpu.CompilerParams(collective_id=0, has_side_effects=True),
        name="heads_exchange",
    )(queries, key_rows, value_rows)


def solution(mesh):
    placed = (P(("dp", "seq"), None), P(("dp", "seq"), None), P(("dp", "seq"), None))
    return jax.shard_map(
        on_device, mesh=mesh, in_specs=placed, out_specs=P("dp", "seq"), check_vma=False
    )
```

```python
import functools
import math

import jax
import jax.numpy as jnp
from jax import lax
from jax.experimental import pallas as pl
from jax.experimental.pallas import tpu as pltpu
from jax.sharding import PartitionSpec as P

HEAD_DIM = 128
GRID_W = 64
MERGE = 2


def by_heads(queries, key_rows, value_rows, score_scale):
    tok_rows, width = queries.shape
    heads = width // HEAD_DIM
    groups = lax.axis_size("seq")
    padded_heads = -(-heads // groups) * groups

    def spread(source):
        shaped = source.reshape(tok_rows, heads, HEAD_DIM)
        shaped = jnp.pad(shaped, ((0, 0), (0, padded_heads - heads), (0, 0)))
        return shaped.reshape(tok_rows, groups, padded_heads // groups, HEAD_DIM)

    head_query = lax.all_to_all(spread(queries), "seq", split_axis=1, concat_axis=0, tiled=True)
    head_key = lax.all_to_all(spread(key_rows), "seq", split_axis=1, concat_axis=0, tiled=True)
    head_value = lax.all_to_all(spread(value_rows), "seq", split_axis=1, concat_axis=0, tiled=True)
    total_rows = head_query.shape[0]
    head_count = head_query.shape[2]
    flat_key = head_key.reshape(total_rows, head_count, HEAD_DIM)
    flat_value = head_value.reshape(total_rows, head_count, HEAD_DIM)
    step_rows = math.gcd(total_rows, 512)
    blocks = head_query.reshape(total_rows // step_rows, step_rows, head_count, HEAD_DIM)

    def one_block(query_block):
        scores = (
            jnp.einsum("qhd,khd->hqk", query_block, flat_key, preferred_element_type=jnp.float32)
            * score_scale
        )
        row_max = jnp.max(scores, axis=-1, keepdims=True)
        weights = jnp.exp(scores - row_max)
        totals = jnp.sum(weights, axis=-1, keepdims=True)
        weighted = jnp.einsum(
            "hqk,khd->qhd",
            weights.astype(jnp.bfloat16),
            flat_value,
            preferred_element_type=jnp.float32,
        )
        return (weighted / totals.transpose(1, 0, 2)).astype(jnp.bfloat16)

    result = lax.map(one_block, blocks).reshape(total_rows, 1, head_count, HEAD_DIM)
    result = lax.all_to_all(result, "seq", split_axis=0, concat_axis=1, tiled=True)
    return result.reshape(tok_rows, padded_heads, HEAD_DIM)[:, :heads].reshape(tok_rows, width)


def split_features(queries, key_rows, value_rows):
    score_scale = 1.0 / math.sqrt(HEAD_DIM)
    attended = by_heads(queries, key_rows, value_rows, score_scale)
    tok_rows, width = attended.shape
    grid_rows = tok_rows // GRID_W
    shuffled = attended.reshape(grid_rows // 2, 2, GRID_W // 2, 2, width).transpose(0, 2, 1, 3, 4)
    shuffled = shuffled.reshape(grid_rows // 2 * (GRID_W // 2), 4 * width)
    return lax.all_to_all(shuffled, "seq", split_axis=1, concat_axis=0, tiled=True)


def head_kernel(
    n, heads, query_rows,
    q_ref, k_ref, v_ref, out_ref,
    held, obuf, osend, staged,
    loaded, landed, sent, merged, ready, far,
):
    me = lax.axis_index("seq")
    inner = (me > 0) & (me < n - 1)
    partner = n - 1 - me
    mate = me + jnp.where(inner, 1, -1) * jnp.where(me < n // 2, -1, 1)

    def tell(sem, device):
        pl.semaphore_signal(
            sem, inc=1, device_id={"seq": device}, device_id_type=pl.DeviceIdType.MESH
        )

    barrier = pltpu.get_barrier_semaphore()

    @pl.when(inner)
    def _():
        tell(barrier, partner)
        tell(barrier, mate)

    flip = lax.rem(lax.axis_index("dp"), 2)
    base, extra = heads // n, heads % n
    lead = 1 if extra else 0
    slots = base + lead
    rows = q_ref.shape[0]
    total_rows = rows * n
    score_scale = 1.0 / math.sqrt(HEAD_DIM)

    def place(device):
        at = device + 1 - 2 * lax.rem(device, 2)
        return flip * (n - 1 - at) + (1 - flip) * at

    def head_of(device, slot):
        at = place(device)
        regular = at * base + slot - lead
        if not lead:
            return regular
        return jnp.where(slot == 0, n * base + at, regular)

    def has(device, slot):
        if not lead:
            return slot >= 0
        return jnp.logical_or(slot > 0, place(device) < extra)

    def columns(head):
        return pl.ds(pl.multiple_of(head * HEAD_DIM, HEAD_DIM), HEAD_DIM)

    def rows_of(tensor, device):
        return pl.ds(pl.multiple_of(tensor * total_rows + device * rows, rows), rows)

    across = me + jnp.where(me < n // 2, n // 2, -(n // 2))
    peers = (partner, across, mate)
    tensors = (k_ref, q_ref, v_ref)

    def group_of(slot):
        return slot - jnp.where(slot >= lead, lead, 0)

    def inward(t, slot, peer, source=None):
        return pltpu.make_async_remote_copy(
            src_ref=tensors[t].at[:, columns(head_of(peer, slot))] if source is None else source,
            dst_ref=held.at[slot, rows_of(t, me), :],
            send_sem=sent,
            recv_sem=landed.at[group_of(slot)],
            device_id={"seq": peer},
            device_id_type=pl.DeviceIdType.MESH,
        )

    def inward_own(t, slot):
        return pltpu.make_async_copy(
            tensors[t].at[:, columns(head_of(me, slot))],
            held.at[slot, rows_of(t, me), :],
            landed.at[group_of(slot)],
        )

    def outward(slot, peer):
        return pltpu.make_async_remote_copy(
            src_ref=osend.at[slot, peer],
            dst_ref=out_ref.at[:, columns(head_of(me, slot))],
            send_sem=sent,
            recv_sem=merged,
            device_id={"seq": peer},
            device_id_type=pl.DeviceIdType.MESH,
        )

    def outward_own(slot):
        return pltpu.make_async_copy(
            osend.at[slot, me], out_ref.at[:, columns(head_of(me, slot))], merged
        )

    def wait_bytes(ref, sem):
        pltpu.make_async_copy(ref, ref, sem).wait()

    far_low = jnp.where(me < n // 2, n // 2, 0)
    far_high = far_low + 1
    early = lead + 1

    left = me == n // 2 - 1

    @pl.when(left)
    def _():
        for t in range(3):
            pltpu.make_async_copy(
                tensors[t].at[:, columns(head_of(partner, lead))], staged.at[t], loaded
            ).start()

    pl.semaphore_wait(barrier, 1)

    @pl.when(inner)
    def _():
        @pl.when(jnp.logical_not(left))
        def _():
            for t in range(3):
                inward(t, lead, partner).start()

        @pl.when(left)
        def _():
            wait_bytes(staged, loaded)
            for t in range(3):
                inward(t, lead, partner, staged.at[t]).start()

        for slot in range(lead):
            for t in range(3):
                @pl.when(has(partner, slot))
                def _():
                    inward(t, slot, partner).start()
        pl.semaphore_wait(ready, 1)
        tell(far, partner)
        pl.semaphore_wait(far, 1)
        tell(far, mate)

    @pl.when(jnp.logical_not(inner))
    def _():
        tell(ready, mate)
        pl.semaphore_wait(far, 1)

    @pl.loop(0, slots)
    def _(slot):
        for t in range(3):
            for peer in peers:
                fresh = has(peer, slot)
                if peer is partner:
                    fresh = fresh & ((slot >= early) | jnp.logical_not(inner))

                @pl.when(fresh)
                def _():
                    inward(t, slot, peer).start()

            @pl.when(has(me, slot))
            def _():
                inward_own(t, slot).start()

    @pl.loop(0, slots)
    def _(slot):
        @pl.when(has(me, slot))
        def _():
            first = has(me, 0) if lead else False

            @pl.when((slot == 0) & first)
            def _():
                wait_bytes(held.at[pl.ds(0, early)], landed.at[0])

            @pl.when((slot == lead) & jnp.logical_not(first))
            def _():
                wait_bytes(held.at[lead], landed.at[0])

            @pl.when(slot > lead)
            def _():
                wait_bytes(held.at[slot], landed.at[group_of(slot)])

            @pl.loop(0, total_rows // query_rows, unroll=2)
            def _(block):
                at = pl.ds(pl.multiple_of(block * query_rows, query_rows), query_rows)
                from_q = pl.ds(pl.multiple_of(total_rows + block * query_rows, query_rows), query_rows)
                scores = lax.dot_general(
                    held[slot, from_q, :], held[slot, pl.ds(0, total_rows), :], (((1,), (1,)), ((), ())),
                    preferred_element_type=jnp.float32,
                ) * score_scale
                row_max = jnp.max(scores, axis=-1, keepdims=True)
                weights = jnp.exp(scores - row_max)
                totals = jnp.sum(weights, axis=-1, keepdims=True)
                weighted = jnp.dot(
                    weights.astype(jnp.bfloat16), held[slot, pl.ds(2 * total_rows, total_rows), :],
                    preferred_element_type=jnp.float32,
                )
                obuf[at, :] = weighted / totals

            half = GRID_W // MERGE
            for a in range(MERGE):
                for b in range(MERGE):
                    for i in range(total_rows // GRID_W // MERGE):
                        part = obuf[pl.ds((MERGE * i + a) * GRID_W + b, half, stride=MERGE), :]
                        osend[slot, MERGE * a + b, i * half:(i + 1) * half, :] = part.astype(jnp.bfloat16)
            outward(slot, mate).start()

            @pl.when(inner)
            def _():
                outward(slot, far_low).start()

            @pl.when(jnp.logical_not(inner))
            def _():
                outward(slot, far_low).start()

            outward_own(slot).start()

    @pl.when(inner)
    def _():
        for peer in (far_high,):
            @pl.loop(0, slots)
            def _(slot):
                @pl.when(has(me, slot))
                def _():
                    outward(slot, peer).start()

    @pl.when(jnp.logical_not(inner))
    def _():
        for peer in (far_high,):
            @pl.loop(0, slots)
            def _(slot):
                @pl.when(has(me, slot))
                def _():
                    outward(slot, peer).start()

    for _ in range(3):
        wait_bytes(q_ref, sent)
    wait_bytes(out_ref, merged)


def on_device(queries, key_rows, value_rows):
    n = lax.axis_size("seq")
    if n != MERGE * MERGE:
        return split_features(queries, key_rows, value_rows)
    rows, width = queries.shape
    heads = width // HEAD_DIM
    slots = -(-heads // n)
    total_rows = rows * n
    merged_rows = total_rows // (MERGE * MERGE)
    anywhere = pl.BlockSpec(memory_space=pl.ANY)
    return pl.pallas_call(
        functools.partial(head_kernel, n, heads, math.gcd(total_rows, 256)),
        out_shape=pltpu.VMEM((merged_rows, width), jnp.bfloat16),
        in_specs=[anywhere] * 3,
        out_specs=pl.BlockSpec(memory_space=pltpu.VMEM),
        scratch_shapes=[
            pltpu.VMEM((slots, 3 * total_rows, HEAD_DIM), jnp.bfloat16),
            pltpu.VMEM((total_rows + 8, HEAD_DIM), jnp.float32),
            pltpu.VMEM((slots, n, merged_rows, HEAD_DIM), jnp.bfloat16),
            pltpu.VMEM((3, rows, HEAD_DIM), jnp.bfloat16),
            pltpu.SemaphoreType.DMA,
            pltpu.SemaphoreType.DMA((heads // n,)),
            pltpu.SemaphoreType.DMA,
            pltpu.SemaphoreType.DMA,
            pltpu.SemaphoreType.REGULAR,
            pltpu.SemaphoreType.REGULAR,
        ],
        compiler_params=pltpu.CompilerParams(collective_id=0, has_side_effects=True),
        name="heads_exchange",
    )(queries, key_rows, value_rows)


def solution(mesh):
    placed = (P(("dp", "seq"), None), P(("dp", "seq"), None), P(("dp", "seq"), None))
    return jax.shard_map(
        on_device, mesh=mesh, in_specs=placed, out_specs=P("dp", "seq"), check_vma=False
    )
```
